8 devices in a mesh: dp: 2 (over z, y), sp: 4 (over x, core).
Axes of the slice: x: 2, y: 2, z: 1, core: 2. Of those that a mesh axis runs over, the one named last changes fastest.
Arguments:
- prompt: bfloat16 [8, 2048, 5120], P('dp', 'sp'), parts along dimension 0
- w_q: bfloat16 [5120, 5120], replicated
- w_k: bfloat16 [5120, 5120], replicated
- w_v: bfloat16 [5120, 5120], replicated
- w_o: bfloat16 [5120, 5120], replicated
- q_norm_w: float32 [5120], replicated
- k_norm_w: float32 [5120], replicated
- post_norm_w: float32 [5120], replicated
- new_token: bfloat16 [8, 5120], P('dp'), parts along dimension 0
Outputs:
- output 1: bfloat16 [8, 2048, 5120], P('dp', 'sp'), parts along dimension 0
- output 2: bfloat16 [8, 2049, 40, 128], P('dp', None, 'sp'), parts along dimension 0
- output 3: bfloat16 [8, 2049, 40, 128], P('dp', None, 'sp'), parts along dimension 0
- output 4: bfloat16 [8, 5120], P('dp'), parts along dimension 0
There are 2 independent parts. The reference program is written for one: setup_inputs(seed, part) draws one part's arguments, and reference() takes and returns one part's arrays. A program takes and returns all parts, laid end to end along the dimension named above; an argument that names none is the same for every part.
All inputs are finite; a program needn't handle non-finite values.
Results may differ from the reference program's by a relative error of at most 0.00819894.
Values are sent between devices in bfloat16 or wider.
A program may use at most 1.25 GiB of HBM per device.

```python
import jax
import jax.numpy as jnp
from jax import lax

BATCH_ROWS = 4
TOKENS_DEV = 512
GROUP_SIZE = 4
MODEL_WIDTH = 5120
NUM_HEADS = 40
HEAD_DIM = 128

SEQ_LEN = TOKENS_DEV * GROUP_SIZE
HEADS_LOCAL = NUM_HEADS // GROUP_SIZE
QUERY_ROWS = min(TOKENS_DEV, 128)
ROPE_THETA = 500000.0
NORM_EPS = 1e-6


def setup_inputs(seed: int = 0, part: int = 0) -> dict:
    base_key = jax.random.key(seed)
    part_key = jax.random.fold_in(base_key, part)
    w_keys = jax.random.split(base_key, 9)
    x_keys = jax.random.split(part_key, 2)
    fan_scale = MODEL_WIDTH ** -0.5
    q_heads = jnp.exp(jax.random.uniform(w_keys[0], (NUM_HEADS,), jnp.float32, -0.5, 0.5))
    k_heads = jnp.exp(jax.random.uniform(w_keys[1], (NUM_HEADS,), jnp.float32, -0.5, 0.5))
    q_cols = jnp.repeat(q_heads, HEAD_DIM) * fan_scale
    k_cols = jnp.repeat(k_heads, HEAD_DIM) * fan_scale
    w_shape = (MODEL_WIDTH, MODEL_WIDTH)
    w_q = (jax.random.normal(w_keys[2], w_shape, jnp.float32) * q_cols[None, :]).astype(jnp.bfloat16)
    w_k = (jax.random.normal(w_keys[3], w_shape, jnp.float32) * k_cols[None, :]).astype(jnp.bfloat16)
    w_v = (jax.random.normal(w_keys[4], w_shape, jnp.float32) * fan_scale).astype(jnp.bfloat16)
    w_o = (jax.random.normal(w_keys[5], w_shape, jnp.float32) * fan_scale).astype(jnp.bfloat16)
    q_norm_w = jax.random.uniform(w_keys[6], (MODEL_WIDTH,), jnp.float32, 0.5, 1.5)
    k_norm_w = jax.random.uniform(w_keys[7], (MODEL_WIDTH,), jnp.float32, 0.5, 1.5)
    post_norm_w = jax.random.uniform(w_keys[8], (MODEL_WIDTH,), jnp.float32, 0.5, 1.5)
    prompt = jax.random.normal(x_keys[0], (BATCH_ROWS, SEQ_LEN, MODEL_WIDTH), jnp.float32).astype(jnp.bfloat16)
    new_token = jax.random.normal(x_keys[1], (BATCH_ROWS, MODEL_WIDTH), jnp.float32).astype(jnp.bfloat16)
    return {"prompt": prompt, "w_q": w_q, "w_k": w_k, "w_v": w_v, "w_o": w_o, "q_norm_w": q_norm_w, "k_norm_w": k_norm_w, "post_norm_w": post_norm_w, "new_token": new_token}


def rms_norm(values, weight):
    return values * lax.rsqrt(jnp.mean(values * values, axis=-1, keepdims=True) + NORM_EPS) * weight


def rope_tables(positions):
    inv_freq = ROPE_THETA ** (-jnp.arange(0, HEAD_DIM, 2).astype(jnp.float32) / HEAD_DIM)
    angles = positions.astype(jnp.float32)[:, None] * inv_freq[None, :]
    angles = jnp.concatenate([angles, angles], axis=-1)
    return jnp.cos(angles), jnp.sin(angles)


def apply_rope(values, cos_t, sin_t):
    half_dim = HEAD_DIM // 2
    rotated = jnp.concatenate([-values[..., half_dim:], values[..., :half_dim]], axis=-1)
    return values * cos_t[:, None, :] + rotated * sin_t[:, None, :]


def project_heads(x_rows, w_mat, norm_w, cos_t, sin_t):
    normed = rms_norm(jnp.dot(x_rows, w_mat, preferred_element_type=jnp.float32), norm_w)
    return apply_rope(normed.reshape(x_rows.shape[0], NUM_HEADS, HEAD_DIM), cos_t, sin_t).astype(jnp.bfloat16)


def one_sequence(prompt_seq, new_row, w_q, w_k, w_v, w_o, q_norm_w, k_norm_w, post_norm_w):
    score_scale = HEAD_DIM ** -0.5
    cos_p, sin_p = rope_tables(jnp.arange(SEQ_LEN))
    q_seq = project_heads(prompt_seq, w_q, q_norm_w, cos_p, sin_p)
    k_seq = project_heads(prompt_seq, w_k, k_norm_w, cos_p, sin_p)
    v_seq = jnp.dot(prompt_seq, w_v, preferred_element_type=jnp.float32).astype(jnp.bfloat16).reshape(SEQ_LEN, NUM_HEADS, HEAD_DIM)
    k_wide = k_seq.astype(jnp.float32)
    v_wide = v_seq.astype(jnp.float32)
    key_pos = jnp.arange(SEQ_LEN)

    def query_block(block_idx):
        q_blk = lax.dynamic_slice_in_dim(q_seq, block_idx * QUERY_ROWS, QUERY_ROWS, axis=0).astype(jnp.float32)
        q_pos = block_idx * QUERY_ROWS + jnp.arange(QUERY_ROWS)
        scores = jnp.einsum("qhd,khd->hqk", q_blk, k_wide) * score_scale
        scores = jnp.where((q_pos[:, None] >= key_pos[None, :])[None], scores, -1e30)
        attn_p = jax.nn.softmax(scores, axis=-1).astype(jnp.bfloat16)
        return jnp.einsum("hqk,khd->qhd", attn_p.astype(jnp.float32), v_wide).astype(jnp.bfloat16)

    attn_out = lax.map(query_block, jnp.arange(SEQ_LEN // QUERY_ROWS)).reshape(SEQ_LEN, MODEL_WIDTH)
    proj_pre = jnp.dot(attn_out, w_o, preferred_element_type=jnp.float32)
    out_p = (prompt_seq.astype(jnp.float32) + rms_norm(proj_pre, post_norm_w)).astype(jnp.bfloat16)
    cos_d, sin_d = rope_tables(jnp.full((1,), SEQ_LEN))
    q_new = project_heads(new_row[None, :], w_q, q_norm_w, cos_d, sin_d)[0]
    k_new = project_heads(new_row[None, :], w_k, k_norm_w, cos_d, sin_d)[0]
    v_new = jnp.dot(new_row[None, :], w_v, preferred_element_type=jnp.float32).astype(jnp.bfloat16).reshape(NUM_HEADS, HEAD_DIM)
    k_cache = jnp.concatenate([k_seq, k_new[None]], axis=0)
    v_cache = jnp.concatenate([v_seq, v_new[None]], axis=0)
    scores_d = jnp.einsum("hd,khd->hk", q_new.astype(jnp.float32), k_cache.astype(jnp.float32)) * score_scale
    attn_d = jax.nn.softmax(scores_d, axis=-1).astype(jnp.bfloat16)
    o_new = jnp.einsum("hk,khd->hd", attn_d.astype(jnp.float32), v_cache.astype(jnp.float32)).astype(jnp.bfloat16)
    o_groups = o_new.reshape(GROUP_SIZE, HEADS_LOCAL * HEAD_DIM).astype(jnp.float32)
    w_groups = w_o.reshape(GROUP_SIZE, HEADS_LOCAL * HEAD_DIM, MODEL_WIDTH).astype(jnp.float32)
    part_proj = jnp.einsum("gc,gcn->gn", o_groups, w_groups).astype(jnp.bfloat16)
    proj_new = jnp.sum(part_proj.astype(jnp.float32), axis=0)
    out_d = (new_row.astype(jnp.float32) + rms_norm(proj_new, post_norm_w)).astype(jnp.bfloat16)
    return out_p, k_cache, v_cache, out_d


def reference(prompt, w_q, w_k, w_v, w_o, q_norm_w, k_norm_w, post_norm_w, new_token):
    out_p, k_cache, v_cache, out_d = lax.map(
        lambda seq_pair: one_sequence(seq_pair[0], seq_pair[1], w_q, w_k, w_v, w_o, q_norm_w, k_norm_w, post_norm_w),
        (prompt, new_token))
    return out_p, k_cache, v_cache, out_d
```

```python
import jax
import jax.numpy as jnp
from jax import lax
from jax.experimental import pallas as pl
from jax.experimental.pallas import tpu as pltpu
from jax.sharding import PartitionSpec as P

HEAD_DIM = 128
ROPE_THETA = 500000.0
NORM_EPS = 1e-6
LOG2E = 1.4426950408889634
BF16 = jnp.bfloat16
F32 = jnp.float32


def rms_norm(values, weight):
    return values * lax.rsqrt(jnp.mean(values * values, axis=-1, keepdims=True) + NORM_EPS) * weight


def rope_tables(positions):
    inv_freq = ROPE_THETA ** (-jnp.arange(0, HEAD_DIM, 2).astype(F32) / HEAD_DIM)
    angles = positions.astype(F32)[:, None] * inv_freq[None, :]
    angles = jnp.concatenate([angles, angles], axis=-1)
    return jnp.cos(angles), jnp.sin(angles)


def apply_rope(values, cos_t, sin_t):
    half_dim = HEAD_DIM // 2
    rotated = jnp.concatenate([-values[..., half_dim:], values[..., :half_dim]], axis=-1)
    return values * cos_t[:, None, :] + rotated * sin_t[:, None, :]


def qkv_kernel(where, wq, wk, wv, x_ref, token_in, q_out, k_out, v_out, sq_out, token):
    step = pl.program_id(1)
    for w_ref, out in ((wq, q_out), (wk, k_out), (wv, v_out)):
        prod = jnp.dot(x_ref[...].reshape(-1, x_ref.shape[-1]), w_ref[...], preferred_element_type=F32)
        out[...] = prod.reshape(out.shape).astype(out.dtype)
    for which, out in enumerate((q_out, k_out)):
        values = out[...].reshape(-1, out.shape[-1])
        lanes = None
        for lo in range(0, values.shape[1], HEAD_DIM):
            piece = values[:, lo:lo + HEAD_DIM] * values[:, lo:lo + HEAD_DIM]
            lanes = piece if lanes is None else lanes + piece
        lanes = lanes.reshape(sq_out.shape[1:])

        @pl.when(step == 0)
        def _():
            sq_out[which] = lanes

        @pl.when(step > 0)
        def _():
            sq_out[which] += lanes
    token[...] = jnp.zeros_like(token)


def project_qkv(name, where, x_all, pairs, weights, token):
    group, (rows, full) = 2, x_all.shape[-2:]
    cols = full // 4
    width = 256
    steps = cols // width
    if pairs is None:
        count, x_map = x_all.shape[0], lambda m, n, s: (m, 0, 0)
    else:
        count, x_map = 2, lambda m, n, s: (s[1], 0, 0)
    out_spec = pl.BlockSpec((group, rows, width), lambda m, n, s: (m, 0, n))
    return pl.pallas_call(
        qkv_kernel,
        grid_spec=pltpu.PrefetchScalarGridSpec(
            num_scalar_prefetch=1, grid=(count // group, steps),
            in_specs=[pl.BlockSpec((full, width), lambda m, n, s: (0, s[0] * steps + n))] * 3
            + [pl.BlockSpec((group, rows, full), x_map), pl.BlockSpec(memory_space=pl.ANY)],
            out_specs=[out_spec] * 3 + [pl.BlockSpec((2, group, rows, HEAD_DIM), lambda m, n, s: (0, m, 0, 0)),
                                        pl.BlockSpec((8, 128), lambda m, n, s: (0, 0))]),
        out_shape=[jax.ShapeDtypeStruct((count, rows, cols), t) for t in (F32, F32, BF16)]
        + [jax.ShapeDtypeStruct((2, count, rows, HEAD_DIM), F32), jax.ShapeDtypeStruct((8, 128), F32)],
        compiler_params=pltpu.CompilerParams(dimension_semantics=("arbitrary", "arbitrary"), vmem_limit_bytes=62 << 20),
        cost_estimate=pl.CostEstimate(flops=6 * count * rows * full * cols, bytes_accessed=70 << 20, transcendentals=0),
        name=name,
    )(where, *weights, x_all, token)


def attention_kernel(slots, q0, q1, q2, q3, k0, k1, k2, k3, v0, v1, v2, v3, r_ref, qg, kg, cos_ref, sin_ref,
                     qn, kn, vn, token_in, o0, o1, o2, o3, kc, vc, od, token, qs, ks, os):
    token[...] = jnp.zeros_like(token)
    rows = q0.shape[0]
    n_all = 4 * rows
    tile = min(256, rows)
    scale = HEAD_DIM ** -0.5 * LOG2E
    for piece, (q_in, k_in, v_in) in enumerate(((q0, k0, v0), (q1, k1, v1), (q2, k2, v2), (q3, k3, v3))):
        at = pl.ds(pl.multiple_of(slots[piece] * rows, rows), rows)
        cos_t, sin_t = cos_ref[at, :], sin_ref[at, :]
        for col, src, gain, dst in ((0, q_in, qg, qs), (1, k_in, kg, ks)):
            normed = src[...] * r_ref[at, col:col + 1] * gain[...]
            dst[at, :] = (normed * cos_t + pltpu.roll(normed, HEAD_DIM // 2, 1) * sin_t).astype(BF16)
        vc[at, :] = v_in[...]
    kc[...] = ks[...]
    contract = (((1,), (1,)), ((), ()))
    row_id = lax.broadcasted_iota(jnp.int32, (tile, tile), 0)
    col_id = lax.broadcasted_iota(jnp.int32, (tile, tile), 1)
    for i in range(n_all // tile):
        lo = i * tile
        q_t = qs[lo:lo + tile, :]
        diag = lax.dot_general(q_t, ks[lo:lo + tile, :], contract, preferred_element_type=F32)
        diag = jnp.where(row_id >= col_id, diag, -1e30)
        peak = jnp.max(diag, axis=1, keepdims=True)
        if i:
            main = lax.dot_general(q_t, ks[0:lo, :], contract, preferred_element_type=F32)
            peak = jnp.maximum(peak, jnp.max(main, axis=1, keepdims=True))
            e_main = jnp.exp2((main - peak) * scale)
        e_diag = jnp.exp2((diag - peak) * scale)
        total = jnp.sum(e_diag, axis=1, keepdims=True)
        if i:
            total = total + jnp.sum(e_main, axis=1, keepdims=True)
        inv = 1.0 / total
        out = jnp.dot((e_diag * inv).astype(BF16), vc[lo:lo + tile, :], preferred_element_type=F32)
        if i:
            out = out + jnp.dot((e_main * inv).astype(BF16), vc[0:lo, :], preferred_element_type=F32)
        os[lo:lo + tile, :] = out.astype(BF16)
    for piece, o_out in enumerate((o0, o1, o2, o3)):
        o_out[...] = os[pl.ds(pl.multiple_of(slots[4 + piece] * rows, rows), rows), :]
    q_n, k_n, v_n = qn[...], kn[...].astype(F32), vn[...].astype(F32)
    s_all = lax.dot_general(q_n, ks[...], contract, preferred_element_type=F32)
    s_new = jnp.sum(q_n.astype(F32) * k_n, axis=1, keepdims=True)
    peak = jnp.maximum(jnp.max(s_all, axis=1, keepdims=True), s_new)
    e_all, e_new = jnp.exp2((s_all - peak) * scale), jnp.exp2((s_new - peak) * scale)
    inv = 1.0 / (jnp.sum(e_all, axis=1, keepdims=True) + e_new)
    out = jnp.dot((e_all * inv).astype(BF16), vc[...], preferred_element_type=F32)
    out = out + (e_new * inv).astype(BF16).astype(F32) * v_n
    od[...] = out.astype(BF16)


def attention(batch, slots, q_parts, k_parts, v_parts, r_inv, q_gain, k_gain, cos_t, sin_t, q_new, k_new, v_new, token):
    rows, cols = q_parts[0][0].shape[-2:]
    n_heads = cols // HEAD_DIM
    n_all = 4 * rows

    def part_spec(index):
        return pl.BlockSpec((None, rows, HEAD_DIM), lambda h, s: (index, 0, h))

    gain_spec = pl.BlockSpec((1, HEAD_DIM), lambda h, s: (0, h))
    table_spec = pl.BlockSpec((n_all, HEAD_DIM), lambda h, s: (0, 0))
    new_spec = pl.BlockSpec((None, 16, HEAD_DIM), lambda h, s: (batch, 0, h))
    parts = [*q_parts, *k_parts, *v_parts]
    work = n_heads * n_all * n_all * HEAD_DIM * 2
    return pl.pallas_call(
        attention_kernel,
        grid_spec=pltpu.PrefetchScalarGridSpec(
            num_scalar_prefetch=1, grid=(n_heads,),
            in_specs=[part_spec(index) for _, index in parts] + [
                pl.BlockSpec((n_all, 2), lambda h, s: (0, 0)), gain_spec, gain_spec, table_spec, table_spec,
                new_spec, new_spec, new_spec, pl.BlockSpec(memory_space=pl.ANY)],
            out_specs=[pl.BlockSpec((rows, HEAD_DIM), lambda h, s: (0, h))] * 4
            + [pl.BlockSpec((n_all, HEAD_DIM), lambda h, s: (0, h))] * 2
            + [pl.BlockSpec((16, HEAD_DIM), lambda h, s: (0, h)), pl.BlockSpec((8, 128), lambda h, s: (0, 0))],
            scratch_shapes=[pltpu.VMEM((n_all, HEAD_DIM), BF16)] * 3),
        out_shape=[jax.ShapeDtypeStruct((rows, cols), BF16)] * 4
        + [jax.ShapeDtypeStruct((n_all, cols), BF16)] * 2
        + [jax.ShapeDtypeStruct((16, cols), BF16), jax.ShapeDtypeStruct((8, 128), F32)],
        compiler_params=pltpu.CompilerParams(dimension_semantics=("arbitrary",), vmem_limit_bytes=60 << 20),
        cost_estimate=pl.CostEstimate(flops=2 * work, bytes_accessed=40 << 20, transcendentals=work // 256),
        name=f"attention_{batch}",
    )(slots, *(array for array, _ in parts), r_inv, q_gain, k_gain, cos_t, sin_t, q_new, k_new, v_new, token)


def out_kernel(slots, o0, o1, o2, o3, w_ref, x_ref, gain, token_in, *rest):
    out_ref, token, acc, sums = rest[-4:]
    token[...] = jnp.zeros_like(token)
    step, n_steps = pl.program_id(0), pl.num_programs(0)
    depth, width = o0.shape[1], w_ref.shape[1]
    total = None
    for piece, o_in in enumerate((o0, o1, o2, o3)):
        at = pl.ds(pl.multiple_of(slots[4 + piece] * depth, depth), depth)
        term = jnp.dot(o_in[...], w_ref[at, :], preferred_element_type=F32)
        total = term if total is None else total + term
    acc[:, pl.ds(pl.multiple_of(step * width, width), width)] = total
    square = jnp.sum(total * total, axis=1, keepdims=True)

    @pl.when(step == 0)
    def _():
        sums[...] = jnp.broadcast_to(square, sums.shape)

    @pl.when(step > 0)
    def _():
        sums[...] += jnp.broadcast_to(square, sums.shape)

    @pl.when(step == n_steps - 1)
    def _():
        full = acc.shape[1]
        inv = lax.rsqrt(sums[:, 0:1] / full + NORM_EPS)
        for lo in range(0, full, width):
            cols = slice(lo, lo + width)
            out_ref[:, cols] = (x_ref[:, cols].astype(F32) + acc[:, cols] * inv * gain[:, cols]).astype(BF16)


def project_out(batch, slots, o_parts, w_o, x_all, gain, token, carried):
    n_batch, rows, full = x_all.shape
    depth = o_parts[0].shape[1]
    width = 512
    in_specs = [pl.BlockSpec((rows, depth), lambda n, s: (0, 0))] * 4 + [
        pl.BlockSpec((full, width), lambda n, s: (0, n)),
        pl.BlockSpec((None, rows, full), lambda n, s: (batch, 0, 0)),
        pl.BlockSpec((1, full), lambda n, s: (0, 0)), pl.BlockSpec(memory_space=pl.ANY)]
    operands = [slots, *o_parts, w_o, x_all, gain, token]
    aliases = {}
    if carried is not None:
        in_specs.append(pl.BlockSpec(memory_space=pl.ANY))
        operands.append(carried)
        aliases = {len(operands) - 1: 0}
    return pl.pallas_call(
        out_kernel,
        grid_spec=pltpu.PrefetchScalarGridSpec(
            num_scalar_prefetch=1, grid=(full // width,), in_specs=in_specs,
            out_specs=[pl.BlockSpec((None, rows, full), lambda n, s: (batch, 0, 0)), pl.BlockSpec((8, 128), lambda n, s: (0, 0))],
            scratch_shapes=[pltpu.VMEM((rows, full), F32), pltpu.VMEM((rows, 128), F32)]),
        out_shape=[jax.ShapeDtypeStruct(x_all.shape, BF16), jax.ShapeDtypeStruct((8, 128), F32)],
        input_output_aliases=aliases,
        compiler_params=pltpu.CompilerParams(dimension_semantics=("arbitrary",), vmem_limit_bytes=60 << 20),
        cost_estimate=pl.CostEstimate(flops=2 * rows * full * full, bytes_accessed=70 << 20, transcendentals=0),
        name=f"project_{batch}",
    )(*operands)


def solution(mesh):
    group_n = mesh.shape["sp"]

    def swap(arr, bit):
        return lax.ppermute(arr, "sp", [(i, i ^ bit) for i in range(group_n)])

    def device_step(prompt_blk, w_q, w_k, w_v, w_o, q_norm_w, k_norm_w, post_norm_w, new_rows):
        n_batch, tok_len, full_width = prompt_blk.shape
        n_heads = full_width // HEAD_DIM
        heads_loc = n_heads // group_n
        cols_loc = heads_loc * HEAD_DIM
        me = lax.axis_index("sp")
        col_start = me * cols_loc
        chip, core = me // 2, me % 2
        far_slot = 2 * (1 - chip)
        slots = jnp.stack([me, me ^ 1, far_slot, far_slot + 1, me, me ^ 1, me ^ 2, me ^ 3]).astype(jnp.int32)
        cos_p, sin_p = rope_tables(jnp.arange(group_n * tok_len))
        sign = jnp.where(jnp.arange(HEAD_DIM) < HEAD_DIM // 2, -1.0, 1.0).astype(F32)
        sin_signed = sin_p * sign[None, :]

        q_gain = lax.dynamic_slice_in_dim(q_norm_w, col_start, cols_loc)[None]
        k_gain = lax.dynamic_slice_in_dim(k_norm_w, col_start, cols_loc)[None]
        weights = (w_q, w_k, w_v)
        where = jnp.stack([me, 1 - chip]).astype(jnp.int32)

        q_d, k_d, v_d = (jnp.dot(new_rows, lax.dynamic_slice_in_dim(w, col_start, cols_loc, axis=1), preferred_element_type=F32)
                         for w in weights)
        v_d = v_d.astype(BF16)
        sq_d = jnp.stack([jnp.sum(q_d * q_d, axis=-1), jnp.sum(k_d * k_d, axis=-1)])
        pad = 128

        def share(b, own, near, far):
            mine, other = jnp.sum(own[3][:, b], axis=-1), jnp.sum(near[3][:, b], axis=-1)
            here = jnp.where(core == 0, jnp.stack([mine, other], axis=1), jnp.stack([other, mine], axis=1))
            there = jnp.sum(far[3], axis=-1)
            sq = jnp.where(chip == 0, jnp.concatenate([here, there], axis=1), jnp.concatenate([there, here], axis=1))
            sq = sq.reshape(2, group_n * tok_len)
            if b == 0:
                sq = jnp.concatenate([sq, jnp.pad(sq_d, ((0, 0), (0, pad - n_batch)))], axis=1)
            half = sq + swap(sq, 1)
            return half + swap(half, 2)

        def inverse(total):
            return jnp.transpose(lax.rsqrt(total / full_width + NORM_EPS))

        token = jnp.zeros((8, 128), F32)
        x_near = swap(prompt_blk, 1)
        x_all = [lax.all_gather(prompt_blk[b], "sp") for b in range(n_batch)]
        own = project_qkv("own", where, prompt_blk, None, weights, token)
        near = project_qkv("near", where, x_near, None, weights, own[4])
        far, total = {}, {}
        token = near[4]
        for b in range(2):
            far[b] = project_qkv(f"far_{b}", where, x_all[b], 1, weights, token)
            token = far[b][4]
            total[b] = share(b, own, near, far[b])
        split = group_n * tok_len
        sq_new, total[0] = total[0][:, split:split + n_batch], total[0][:, :split]

        cos_d, sin_d = rope_tables(jnp.full((1,), tok_len * group_n))

        def new_heads(raw, sq, gain):
            scaled = raw * lax.rsqrt(sq[:, None] / full_width + NORM_EPS) * gain
            roped = apply_rope(scaled.reshape(n_batch, heads_loc, HEAD_DIM), cos_d, sin_d)
            return roped.astype(BF16).reshape(n_batch, cols_loc)

        q_new, k_new = new_heads(q_d, sq_new[0], q_gain), new_heads(k_d, sq_new[1], k_gain)

        def widen(row):
            return jnp.broadcast_to(row[:, None], (n_batch, 16, cols_loc))

        new_args = (widen(q_new), widen(k_new), widen(v_d))
        k_rows, v_rows, o_new, o_parts = [], [], [], []
        out_p = None
        for b in range(n_batch):
            parts = [[(own[i], b), (near[i], b), (far[b][i], 0), (far[b][i], 1)] for i in range(3)]
            res = attention(b, slots, *parts, inverse(total[b]), q_gain, k_gain, cos_p, sin_signed, *new_args, token)
            token = res[7]
            o_parts.append((res[0], swap(res[1], 1), swap(res[2], 2), swap(res[3], 3)))
            k_rows.append(res[4])
            v_rows.append(res[5])
            o_new.append(res[6][0])
            if b + 2 < n_batch:
                far[b + 2] = project_qkv(f"far_{b + 2}", where, x_all[b + 2], 1, weights, token)
                token = far[b + 2][4]
                total[b + 2] = share(b + 2, own, near, far[b + 2])
            if b >= 1:
                out_p, token = project_out(b - 1, slots, o_parts[b - 1], w_o, prompt_blk, post_norm_w[None], token, out_p)
        out_p, token = project_out(n_batch - 1, slots, o_parts[n_batch - 1], w_o, prompt_blk, post_norm_w[None], token, out_p)

        def cache(rows, new):
            full = jnp.stack([jnp.concatenate([r, n[None]], axis=0) for r, n in zip(rows, new)])
            return full.reshape(n_batch, -1, heads_loc, HEAD_DIM)

        k_cache, v_cache = cache(k_rows, k_new), cache(v_rows, v_d)

        part_proj = jnp.dot(jnp.stack(o_new), lax.dynamic_slice_in_dim(w_o, col_start, cols_loc, axis=0), preferred_element_type=F32).astype(BF16)
        all_parts = lax.all_gather(part_proj, "sp")
        proj_new = jnp.sum(all_parts.astype(F32), axis=0)
        out_d = (new_rows.astype(F32) + rms_norm(proj_new, post_norm_w)).astype(BF16)
        return out_p, k_cache, v_cache, out_d

    replicated = P()
    return jax.shard_map(
        device_step, mesh=mesh,
        in_specs=(P("dp", "sp", None), replicated, replicated, replicated, replicated, replicated, replicated, replicated, P("dp", None)),
        out_specs=(P("dp", "sp", None), P("dp", None, "sp", None), P("dp", None, "sp", None), P("dp", None)),
        check_vma=False)
```

```python
import functools

import jax
import jax.numpy as jnp
from jax import lax
from jax.experimental import pallas as pl
from jax.experimental.pallas import tpu as pltpu
from jax.sharding import PartitionSpec as P


HEAD_DIM = 128
ROPE_THETA = 500000.0
NORM_EPS = 1e-6
LOG2E = 1.4426950408889634
BF16 = jnp.bfloat16
F32 = jnp.float32


def rms_norm(values, weight):
    return values * lax.rsqrt(jnp.mean(values * values, axis=-1, keepdims=True) + NORM_EPS) * weight


def rope_tables(positions):
    inv_freq = ROPE_THETA ** (-jnp.arange(0, HEAD_DIM, 2).astype(F32) / HEAD_DIM)
    angles = positions.astype(F32)[:, None] * inv_freq[None, :]
    angles = jnp.concatenate([angles, angles], axis=-1)
    return jnp.cos(angles), jnp.sin(angles)


def apply_rope(values, cos_t, sin_t):
    half_dim = HEAD_DIM // 2
    rotated = jnp.concatenate([-values[..., half_dim:], values[..., :half_dim]], axis=-1)
    return values * cos_t[:, None, :] + rotated * sin_t[:, None, :]


def qkv_kernel(where, wq, wk, wv, x_ref, token_in, *rest):
    (q_out, k_out, v_out, sq_out, token), few = rest[-8:-3] if len(rest) > 5 else rest, rest[-3:]
    step = pl.program_id(1)
    for w_ref, out in ((wq, q_out), (wk, k_out), (wv, v_out)):
        prod = jnp.dot(x_ref[...].reshape(-1, x_ref.shape[-1]), w_ref[...], preferred_element_type=F32)
        out[...] = prod.reshape(out.shape).astype(out.dtype)
    for which, out in enumerate((q_out, k_out)):
        values = out[...].reshape(-1, out.shape[-1])
        lanes = None
        for lo in range(0, values.shape[1], HEAD_DIM):
            piece = values[:, lo:lo + HEAD_DIM] * values[:, lo:lo + HEAD_DIM]
            lanes = piece if lanes is None else lanes + piece
        lanes = lanes.reshape(sq_out.shape[1:])

        @pl.when(step == 0)
        def _():
            sq_out[which] = lanes

        @pl.when(step > 0)
        def _():
            sq_out[which] += lanes
    token[...] = jnp.zeros_like(token)
    if len(rest) > 5:
        for w_ref, out in zip((wq, wk, wv), few):
            out[...] = jnp.dot(rest[0][...], w_ref[...], preferred_element_type=F32)


def project_qkv(where, x_all, pairs, weights, token, few=None):
    group, (rows, full) = 2, x_all.shape[-2:]
    cols = full // 4
    width = 256
    steps = cols // width
    if pairs is None:
        count, x_map = x_all.shape[0], lambda m, n, s: (m, 0, 0)
    else:
        count, x_map = 2, lambda m, n, s: (s[1], 0, 0)
    out_spec = pl.BlockSpec((group, rows, width), lambda m, n, s: (m, 0, n))
    more = [] if few is None else [few]
    few_in = [pl.BlockSpec((r.shape[0], full), lambda m, n, s: (0, 0)) for r in more]
    few_out = [pl.BlockSpec((r.shape[0], width), lambda m, n, s: (0, n)) for r in more] * 3
    few_shape = [jax.ShapeDtypeStruct((r.shape[0], cols), F32) for r in more] * 3
    return pl.pallas_call(
        qkv_kernel,
        grid_spec=pltpu.PrefetchScalarGridSpec(
            num_scalar_prefetch=1, grid=(count // group, steps),
            in_specs=[pl.BlockSpec((full, width), lambda m, n, s: (0, s[0] * steps + n))] * 3
            + [pl.BlockSpec((group, rows, full), x_map), pl.BlockSpec(memory_space=pl.ANY)] + few_in,
            out_specs=[out_spec] * 3 + [pl.BlockSpec((2, group, rows, HEAD_DIM), lambda m, n, s: (0, m, 0, 0)),
                                        pl.BlockSpec((8, 128), lambda m, n, s: (0, 0))] + few_out),
        out_shape=[jax.ShapeDtypeStruct((count, rows, cols), t) for t in (F32, F32, BF16)]
        + [jax.ShapeDtypeStruct((2, count, rows, HEAD_DIM), F32), jax.ShapeDtypeStruct((8, 128), F32)] + few_shape,
        compiler_params=pltpu.CompilerParams(dimension_semantics=("arbitrary", "arbitrary"), vmem_limit_bytes=62 << 20),
        cost_estimate=pl.CostEstimate(flops=6 * count * rows * full * cols, bytes_accessed=70 << 20, transcendentals=0),
    )(where, *weights, x_all, token, *more)


def attention_kernel(slots, q0, q1, q2, q3, k0, k1, k2, k3, v0, v1, v2, v3, r_ref, qg, kg, cos_ref, sin_ref,
                     qn, kn, vn, token_in, o0, o1, o2, o3, kc, vc, od, token, qs, os, s_buf, p_buf):
    token[...] = jnp.zeros_like(token)
    rows = q0.shape[0]
    n_all = 4 * rows
    tile = min(256, rows)
    n_tiles = n_all // tile
    scale = HEAD_DIM ** -0.5 * LOG2E
    chunk = min(64, rows)
    for piece, (q_in, k_in, v_in) in enumerate(((q0, k0, v0), (q1, k1, v1), (q2, k2, v2), (q3, k3, v3))):
        start = slots[piece] * rows
        for lo in range(0, rows, chunk):
            at = pl.ds(pl.multiple_of(start + lo, chunk), chunk)
            cos_t, sin_t = cos_ref[at, :], sin_ref[at, :]
            for col, src, gain, dst in ((0, q_in, qg, qs), (1, k_in, kg, kc)):
                normed = src[lo:lo + chunk, :] * r_ref[at, col:col + 1] * gain[...]
                dst[at, :] = (normed * cos_t + pltpu.roll(normed, HEAD_DIM // 2, 1) * sin_t).astype(BF16)
        vc[pl.ds(pl.multiple_of(start, rows), rows), :] = v_in[...]
    contract = (((1,), (1,)), ((), ()))
    row_id = lax.broadcasted_iota(jnp.int32, (tile, tile), 0)
    col_id = lax.broadcasted_iota(jnp.int32, (tile, tile), 1)

    def score(i, j):
        s = lax.dot_general(qs[i * tile:(i + 1) * tile, :], kc[j * tile:(j + 1) * tile, :], contract, preferred_element_type=F32)
        s_buf[i % 2, :, j * tile:(j + 1) * tile] = jnp.where(row_id >= col_id, s, -1e30) if i == j else s

    part = 32

    def soften(i, r, inv):
        cols = range(0, (i + 1) * tile, HEAD_DIM)
        peak = None
        for c in cols:
            s = s_buf[i % 2, r:r + part, c:c + HEAD_DIM]
            peak = s if peak is None else jnp.maximum(peak, s)
        peak = jnp.max(peak, axis=1, keepdims=True) * scale
        total = None
        for c in cols:
            e = jnp.exp2(s_buf[i % 2, r:r + part, c:c + HEAD_DIM] * scale - peak)
            total = e if total is None else total + e
            p_buf[i % 2, r:r + part, c:c + HEAD_DIM] = e.astype(BF16)
        inv.append(1.0 / jnp.sum(total, axis=1, keepdims=True))

    def weigh(i, inv):
        out = jnp.dot(p_buf[i % 2, :, :(i + 1) * tile], vc[:(i + 1) * tile, :], preferred_element_type=F32)
        for at, r in enumerate(range(0, tile, part)):
            os[i * tile + r:i * tile + r + part, :] = (out[r:r + part] * inv[at]).astype(BF16)

    score(0, 0)
    before = None
    for i in range(n_tiles):
        inv = []
        matrix_work = []
        if before is not None:
            matrix_work.append(lambda i=i, done=before: weigh(i - 1, done))
        if i + 1 < n_tiles:
            matrix_work += [lambda i=i, j=j: score(i + 1, j) for j in range(i + 2)]
        starts = list(range(0, tile, part))
        for at, r in enumerate(starts):
            for work in matrix_work[len(matrix_work) * at // len(starts):len(matrix_work) * (at + 1) // len(starts)]:
                work()
            soften(i, r, inv)
        before = inv
    weigh(n_tiles - 1, before)

    for piece, o_out in enumerate((o0, o1, o2, o3)):
        o_out[...] = os[pl.ds(pl.multiple_of(slots[4 + piece] * rows, rows), rows), :]
    q_n, k_n, v_n = qn[...], kn[...].astype(F32), vn[...].astype(F32)
    s_all = lax.dot_general(q_n, kc[...], contract, preferred_element_type=F32)
    s_new = jnp.sum(q_n.astype(F32) * k_n, axis=1, keepdims=True)
    peak = jnp.maximum(jnp.max(s_all, axis=1, keepdims=True), s_new)
    e_all, e_new = jnp.exp2((s_all - peak) * scale), jnp.exp2((s_new - peak) * scale)
    inv = 1.0 / (jnp.sum(e_all, axis=1, keepdims=True) + e_new)
    out = jnp.dot((e_all * inv).astype(BF16), vc[...], preferred_element_type=F32)
    out = out + (e_new * inv).astype(BF16).astype(F32) * v_n
    od[...] = out.astype(BF16)


def attention(batch, slots, q_parts, k_parts, v_parts, r_inv, q_gain, k_gain, cos_t, sin_t, q_new, k_new, v_new, token):
    rows, cols = q_parts[0][0].shape[-2:]
    n_heads = cols // HEAD_DIM
    n_all = 4 * rows

    def part_spec(index):
        return pl.BlockSpec((None, rows, HEAD_DIM), lambda h, s: (index, 0, h))

    gain_spec = pl.BlockSpec((1, HEAD_DIM), lambda h, s: (0, h))
    table_spec = pl.BlockSpec((n_all, HEAD_DIM), lambda h, s: (0, 0))
    new_spec = pl.BlockSpec((None, 16, HEAD_DIM), lambda h, s: (batch, 0, h))
    parts = [*q_parts, *k_parts, *v_parts]
    work = n_heads * n_all * n_all * HEAD_DIM * 2
    return pl.pallas_call(
        attention_kernel,
        grid_spec=pltpu.PrefetchScalarGridSpec(
            num_scalar_prefetch=1, grid=(n_heads,),
            in_specs=[part_spec(index) for _, index in parts] + [
                pl.BlockSpec((n_all, 2), lambda h, s: (0, 0)), gain_spec, gain_spec, table_spec, table_spec,
                new_spec, new_spec, new_spec, pl.BlockSpec(memory_space=pl.ANY)],
            out_specs=[pl.BlockSpec((rows, HEAD_DIM), lambda h, s: (0, h))] * 4
            + [pl.BlockSpec((n_all, HEAD_DIM), lambda h, s: (0, h))] * 2
            + [pl.BlockSpec((16, HEAD_DIM), lambda h, s: (0, h)), pl.BlockSpec((8, 128), lambda h, s: (0, 0))],
            scratch_shapes=[pltpu.VMEM((n_all, HEAD_DIM), BF16)] * 2
            + [pltpu.VMEM((2, min(256, rows), n_all), t) for t in (F32, BF16)]),
        out_shape=[jax.ShapeDtypeStruct((rows, cols), BF16)] * 4
        + [jax.ShapeDtypeStruct((n_all, cols), BF16)] * 2
        + [jax.ShapeDtypeStruct((16, cols), BF16), jax.ShapeDtypeStruct((8, 128), F32)],
        compiler_params=pltpu.CompilerParams(dimension_semantics=("arbitrary",), vmem_limit_bytes=60 << 20),
        cost_estimate=pl.CostEstimate(flops=2 * work, bytes_accessed=40 << 20, transcendentals=work // 256),
    )(slots, *(array for array, _ in parts), r_inv, q_gain, k_gain, cos_t, sin_t, q_new, k_new, v_new, token)


def out_kernel(n_dots, slots, *refs):
    o_refs, (w_ref, x_ref, gain), (out_ref, token, acc, sums, joined, sems) = refs[:8], refs[8:11], refs[-6:]
    token[...] = jnp.zeros_like(token)
    step = pl.program_id(0)
    rows, depth = o_refs[0].shape
    full, width, final = acc.shape[1], w_ref.shape[1], out_ref.shape[-1]

    @pl.when(step == 0)
    def _():
        copies = []
        for at, o_in in enumerate(o_refs):
            cols = pl.ds(pl.multiple_of(slots[4 + at % 4] * depth, depth), depth)
            copies.append(pltpu.make_async_copy(o_in, joined.at[pl.ds(at // 4 * rows, rows), cols], sems.at[at]))
        for copy in copies:
            copy.start()
        sums[...] = jnp.zeros_like(sums)
        for copy in copies:
            copy.wait()

    @pl.when(step < n_dots)
    def _():
        total = jnp.dot(joined[...], w_ref[...], preferred_element_type=F32)
        acc[:, pl.ds(pl.multiple_of(step * width, width), width)] = total
        lanes = sums[...]
        for lo in range(0, width, 128):
            lanes = lanes + total[:, lo:lo + 128] * total[:, lo:lo + 128]
        sums[...] = lanes

    @pl.when(step == n_dots - 1)
    def _():
        inv = lax.rsqrt(jnp.sum(sums[...], axis=1, keepdims=True) / full + NORM_EPS)
        sums[...] = jnp.broadcast_to(inv, sums.shape)

    @pl.when(step >= n_dots)
    def _():
        cols = pl.ds(pl.multiple_of((step - n_dots) * final, final), final)
        for pair in range(2):
            at = slice(pair * rows, (pair + 1) * rows)
            out_ref[pair] = (x_ref[pair].astype(F32) + acc[at, cols] * sums[at, 0:1] * gain[:, cols]).astype(BF16)


def project_out(pair, slots, o_parts, w_o, x_all, gain, token, carried):
    _, rows, full = x_all.shape
    width, final = 512, 1024
    n_dots, n_ends = full // width, full // final
    any_spec = pl.BlockSpec(memory_space=pl.ANY)
    end_spec = pl.BlockSpec((2, rows, final), lambda n, s: (pair, 0, jnp.maximum(n - n_dots, 0)))
    in_specs = [any_spec] * 8 + [
        pl.BlockSpec((full, width), lambda n, s: (0, jnp.minimum(n, n_dots - 1))), end_spec,
        pl.BlockSpec((1, full), lambda n, s: (0, 0)), any_spec]
    operands = [slots, *o_parts, w_o, x_all, gain, token]
    aliases = {}
    if carried is not None:
        in_specs.append(any_spec)
        operands.append(carried)
        aliases = {len(operands) - 1: 0}
    return pl.pallas_call(
        functools.partial(out_kernel, n_dots),
        grid_spec=pltpu.PrefetchScalarGridSpec(
            num_scalar_prefetch=1, grid=(n_dots + n_ends,), in_specs=in_specs,
            out_specs=[end_spec, pl.BlockSpec((8, 128), lambda n, s: (0, 0))],
            scratch_shapes=[pltpu.VMEM((2 * rows, full), F32), pltpu.VMEM((2 * rows, 128), F32),
                            pltpu.VMEM((2 * rows, full), BF16), pltpu.SemaphoreType.DMA((8,))]),
        out_shape=[jax.ShapeDtypeStruct(x_all.shape, BF16), jax.ShapeDtypeStruct((8, 128), F32)],
        input_output_aliases=aliases,
        compiler_params=pltpu.CompilerParams(dimension_semantics=("arbitrary",), vmem_limit_bytes=62 << 20),
        cost_estimate=pl.CostEstimate(flops=4 * rows * full * full, bytes_accessed=90 << 20, transcendentals=0),
    )(*operands)


def cache_kernel(*refs):
    k_rows, v_rows, (k_new, v_new, token_in, k_out, v_out, token, wide) = refs[:4], refs[4:8], refs[8:]
    token[...] = jnp.zeros_like(token)
    last = pl.program_id(0) == pl.num_programs(0) - 1
    block, n_heads, n_batch = k_out.shape[:3]

    @pl.when(jnp.logical_not(last))
    def _():
        for rows, out in ((k_rows, k_out), (v_rows, v_out)):
            for h in range(n_heads):
                for b, row in enumerate(rows):
                    wide[h, pl.ds(b, block, stride=n_batch), :] = row[:, h * HEAD_DIM:(h + 1) * HEAD_DIM].astype(F32)
                out[:, h] = wide[h].reshape(block, n_batch, HEAD_DIM).astype(BF16)

    @pl.when(last)
    def _():
        k_out[0] = k_new[...]
        v_out[0] = v_new[...]


def fill_caches(k_rows, v_rows, k_new, v_new, token):
    n_batch, (n_all, cols) = len(k_rows), k_rows[0].shape
    n_heads = cols // HEAD_DIM
    block = 128
    steps = n_all // block
    row_spec = pl.BlockSpec((block, cols), lambda i: (jnp.minimum(i, steps - 1), 0))
    new_spec = pl.BlockSpec((n_heads, n_batch, HEAD_DIM), lambda i: (0, 0, 0))
    out_spec = pl.BlockSpec((block, n_heads, n_batch, HEAD_DIM), lambda i: (i, 0, 0, 0))
    k_out, v_out, token = pl.pallas_call(
        cache_kernel, grid=(steps + 1,),
        in_specs=[row_spec] * (2 * n_batch) + [new_spec] * 2 + [pl.BlockSpec(memory_space=pl.ANY)],
        out_specs=[out_spec] * 2 + [pl.BlockSpec((8, 128), lambda i: (0, 0))],
        out_shape=[jax.ShapeDtypeStruct((n_all + 1, n_heads, n_batch, HEAD_DIM), BF16)] * 2
        + [jax.ShapeDtypeStruct((8, 128), F32)],
        scratch_shapes=[pltpu.VMEM((n_heads, block * n_batch, HEAD_DIM), F32)],
        compiler_params=pltpu.CompilerParams(dimension_semantics=("arbitrary",)),
        cost_estimate=pl.CostEstimate(flops=0, bytes_accessed=90 << 20, transcendentals=0),
        name="caches",
    )(*k_rows, *v_rows, k_new, v_new, token)
    return jnp.transpose(k_out, (2, 0, 1, 3)), jnp.transpose(v_out, (2, 0, 1, 3)), token


def solution(mesh):
    group_n = mesh.shape["sp"]

    def swap(arr, bit):
        return lax.ppermute(arr, "sp", [(i, i ^ bit) for i in range(group_n)])

    def device_step(prompt_blk, w_q, w_k, w_v, w_o, q_norm_w, k_norm_w, post_norm_w, new_rows):
        n_batch, tok_len, full_width = prompt_blk.shape
        n_heads = full_width // HEAD_DIM
        heads_loc = n_heads // group_n
        cols_loc = heads_loc * HEAD_DIM
        me = lax.axis_index("sp")
        col_start = me * cols_loc
        chip, core = me // 2, me % 2
        far_slot = 2 * (1 - chip)
        slots = jnp.stack([me, me ^ 1, far_slot, far_slot + 1, me, me ^ 1, me ^ 2, me ^ 3]).astype(jnp.int32)
        cos_p, sin_p = rope_tables(jnp.arange(group_n * tok_len))
        sign = jnp.where(jnp.arange(HEAD_DIM) < HEAD_DIM // 2, -1.0, 1.0).astype(F32)
        sin_signed = sin_p * sign[None, :]

        q_gain = lax.dynamic_slice_in_dim(q_norm_w, col_start, cols_loc)[None]
        k_gain = lax.dynamic_slice_in_dim(k_norm_w, col_start, cols_loc)[None]
        weights = (w_q, w_k, w_v)
        where = jnp.stack([me, 1 - chip]).astype(jnp.int32)

        pad = 128

        def share(b, own, near, far, sq_d=None):
            mine, other = jnp.sum(own[3][:, b], axis=-1), jnp.sum(near[3][:, b], axis=-1)
            here = jnp.where(core == 0, jnp.stack([mine, other], axis=1), jnp.stack([other, mine], axis=1))
            there = jnp.sum(far[3], axis=-1)
            sq = jnp.where(chip == 0, jnp.concatenate([here, there], axis=1), jnp.concatenate([there, here], axis=1))
            sq = sq.reshape(2, group_n * tok_len)
            if b == 0:
                sq = jnp.concatenate([sq, jnp.pad(sq_d, ((0, 0), (0, pad - n_batch)))], axis=1)
            half = sq + swap(sq, 1)
            return half + swap(half, 2)

        def inverse(total):
            return jnp.transpose(lax.rsqrt(total / full_width + NORM_EPS))

        token = jnp.zeros((8, 128), F32)
        x_near = swap(prompt_blk, 1)
        x_all = [lax.all_gather(prompt_blk[b], "sp") for b in range(n_batch)]
        own = project_qkv(where, prompt_blk, None, weights, token)
        near = project_qkv(where, x_near, None, weights, own[4])
        far, total = {}, {}
        token = near[4]
        for b in range(2):
            few = jnp.pad(new_rows, ((0, 16 - n_batch), (0, 0))) if b == 0 else None
            far[b] = project_qkv(where, x_all[b], 1, weights, token, few)
            token = far[b][4]
            if b == 0:
                q_d, k_d, v_d = (d[:n_batch] for d in far[b][5:])
                v_d = v_d.astype(BF16)
                sq_d = jnp.stack([jnp.sum(q_d * q_d, axis=-1), jnp.sum(k_d * k_d, axis=-1)])
            total[b] = share(b, own, near, far[b], sq_d)
        split = group_n * tok_len
        sq_new, total[0] = total[0][:, split:split + n_batch], total[0][:, :split]

        cos_d, sin_d = rope_tables(jnp.full((1,), tok_len * group_n))

        def new_heads(raw, sq, gain):
            scaled = raw * lax.rsqrt(sq[:, None] / full_width + NORM_EPS) * gain
            roped = apply_rope(scaled.reshape(n_batch, heads_loc, HEAD_DIM), cos_d, sin_d)
            return roped.astype(BF16).reshape(n_batch, cols_loc)

        q_new, k_new = new_heads(q_d, sq_new[0], q_gain), new_heads(k_d, sq_new[1], k_gain)

        def widen(row):
            return jnp.broadcast_to(row[:, None], (n_batch, 16, cols_loc))

        new_args = (widen(q_new), widen(k_new), widen(v_d))
        k_rows, v_rows, o_new, o_parts = [], [], [], []
        out_p = None

        def attend(b, token):
            parts = [[(own[i], b), (near[i], b), (far[b][i], 0), (far[b][i], 1)] for i in range(3)]
            res = attention(b, slots, *parts, inverse(total[b]), q_gain, k_gain, cos_p, sin_signed, *new_args, token)
            moved = []
            for bit in (2, 3, 1):
                moved.append(swap(res[bit], bit))
            o_parts.append((res[0], moved[2], moved[0], moved[1]))
            k_rows.append(res[4])
            v_rows.append(res[5])
            o_new.append(res[6][0])
            return res[7]

        def project_far(b, token):
            far[b] = project_qkv(where, x_all[b], 1, weights, token)
            total[b] = share(b, own, near, far[b])
            return far[b][4]

        def finish(pair, token):
            parts = (*o_parts[2 * pair], *o_parts[2 * pair + 1])
            return project_out(pair, slots, parts, w_o, prompt_blk, post_norm_w[None], token, out_p)

        token = attend(0, token)
        token = project_far(2, token)
        token = attend(1, token)
        token = attend(2, token)
        token = project_far(3, token)
        out_p, token = finish(0, token)
        token = attend(3, token)

        part_proj = jnp.dot(jnp.stack(o_new), lax.dynamic_slice_in_dim(w_o, col_start, cols_loc, axis=0), preferred_element_type=F32).astype(BF16)
        others = [swap(part_proj, bit).astype(F32) for bit in (1, 2, 3)]
        proj_new = (part_proj.astype(F32) + others[0]) + (others[1] + others[2])
        out_d = (new_rows.astype(F32) + rms_norm(proj_new, post_norm_w)).astype(BF16)

        def per_head(new):
            return jnp.transpose(new.reshape(n_batch, heads_loc, HEAD_DIM), (1, 0, 2))

        k_cache, v_cache, token = fill_caches(k_rows, v_rows, per_head(k_new), per_head(v_d), token)
        out_p, token = finish(1, token)
        return out_p, k_cache, v_cache, out_d

    replicated = P()
    return jax.shard_map(
        device_step, mesh=mesh,
        in_specs=(P("dp", "sp", None), replicated, replicated, replicated, replicated, replicated, replicated, replicated, P("dp", None)),
        out_specs=(P("dp", "sp", None), P("dp", None, "sp", None), P("dp", None, "sp", None), P("dp", None)),
        check_vma=False)
```
